32 devices in a mesh: seq: 8 (over z, core), head: 4 (over y, x).
Axes of the slice: x: 2, y: 2, z: 4, core: 2. Of those that a mesh axis runs over, the one named last changes fastest.
Arguments:
- queries: bfloat16 [4096, 16, 128], P(('seq', 'head')), may hold values from -6 to 6
- keys: bfloat16 [4096, 16, 128], P(('seq', 'head')), may hold values from -6 to 6
- values: bfloat16 [4096, 16, 128], P(('seq', 'head')), may hold values from -6 to 6
- beta: float32 [4096, 16], P(('seq', 'head')), may hold values from 0 to 1
- log_decay: float32 [4096, 16], P(('seq', 'head')), may hold values from -1 to 0
- out_gate: bfloat16 [4096, 16, 128], P(('seq', 'head')), may hold values from -6 to 6
- norm_gain: float32 [128], replicated, may hold values from 0.1 to 1.9
Outputs:
- gated_out: bfloat16 [4096, 16, 128], P('seq', 'head')
The draws below stay inside these ranges and needn't reach their ends.
All inputs are finite; a program needn't handle non-finite values.
Results may differ from the reference program's by a relative error of at most 0.001.
Values may be sent and summed in bfloat16 or wider, within the bound.
A program may use at most 64 MiB of HBM per device.

```python
import jax
import jax.numpy as jnp
from jax import lax

HK = 16
HV = 16
DK = 128
DV = 128
BLOCK = 128
TOK_DEV = 128
PROMPT_LENGTH = 4096


def head_kinds(key):
    slow_share = 5
    return jax.random.randint(jax.random.fold_in(key, 7), (HV,), 0, 10) < slow_share


def draw_beta(key, part):
    slow_heads = head_kinds(key)
    key_one, key_two, key_three = jax.random.split(jax.random.fold_in(key, 21), 3)
    lowest = 0.5 * DK / PROMPT_LENGTH
    slow_level = lowest * jnp.exp(jax.random.uniform(key_one, (HV,), minval=0.0, maxval=jnp.log(2.0)))
    fast_level = jnp.exp(jax.random.uniform(key_two, (HV,), minval=jnp.log(0.05), maxval=jnp.log(0.9)))
    head_level = jnp.where(slow_heads, slow_level, fast_level)
    roughness_measure = jax.random.uniform(key_three, (PROMPT_LENGTH, HV), minval=0.5, maxval=1.0)
    return (head_level[None, :] * roughness_measure).astype(jnp.float32)


def draw_log_decay(key, part):
    slow_heads = head_kinds(key)
    key_one, key_two, key_three, key_four, random_seed_five, random_seed_six = jax.random.split(jax.random.fold_in(key, 33), 6)
    slow_rate = 0.1 / PROMPT_LENGTH * jnp.exp(jax.random.uniform(key_one, (HV,), minval=0.0, maxval=jnp.log(5.0)))
    fast_rate = jnp.exp(jax.random.uniform(key_two, (HV,), minval=jnp.log(0.02), maxval=jnp.log(0.05)))
    steady_speed = jnp.where(slow_heads, slow_rate, fast_rate)
    roughness_measure = jnp.exp(jax.random.uniform(key_three, (PROMPT_LENGTH, HV), minval=jnp.log(0.5), maxval=jnp.log(2.0)))
    shard_division = jnp.exp(jax.random.uniform(key_four, (PROMPT_LENGTH // TOK_DEV, 1), minval=jnp.log(0.5), maxval=jnp.log(2.0)))
    shard_division = jnp.repeat(shard_division, TOK_DEV, axis=0)
    spike_location = jax.random.randint(random_seed_five, (6,), 0, PROMPT_LENGTH)
    spike_height = jax.random.uniform(random_seed_six, (6,), minval=0.2, maxval=0.7)
    spike_influence = lax.broadcasted_iota(jnp.int32, (PROMPT_LENGTH, 6), 0) == spike_location[None, :]
    spike_charge = jnp.minimum(jnp.sum(jnp.where(spike_influence, spike_height[None, :], 0.0), axis=1), 0.7)
    overall_summation = -(steady_speed[None, :] * roughness_measure * shard_division) - spike_charge[:, None]
    return jnp.maximum(overall_summation, -1.0).astype(jnp.float32)


def level_of(stream_key, shape, shards, low, high):
    def one(position, parts):
        heights = jax.random.uniform(jax.random.fold_in(jax.random.fold_in(stream_key, 6), position), (parts,), jnp.float32, low / len(shards), high / len(shards))
        return jnp.repeat(jnp.exp(heights), shape[position] // parts).reshape((-1,) + (1,) * (len(shape) - position - 1))

    gain = one(*shards[0])
    for cut in shards[1:]:
        gain = gain * one(*cut)
    return gain


def scatter_about(own_key, dims, scale, limit, shards=(), kind=jnp.bfloat16):
    gain = level_of(own_key, dims, shards, -0.22, 0.18) if shards else 1.0
    entries = jax.random.normal(own_key, dims, jnp.float32) * scale * gain
    return jnp.minimum(jnp.maximum(entries, -limit), limit).astype(kind)


def setup_inputs(seed: int = 0) -> dict:
    seeds = jax.random.split(jax.random.key(seed), 8)
    return {
        "queries": scatter_about(seeds[0], (PROMPT_LENGTH, HK, DK), 1.0, 6.0, ((0, 32),)),
        "keys": scatter_about(seeds[1], (PROMPT_LENGTH, HK, DK), 1.0, 6.0, ((0, 32),)),
        "values": scatter_about(seeds[2], (PROMPT_LENGTH, HV, DV), 1.0, 6.0, ((0, 32),)),
        "beta": draw_beta(jax.random.fold_in(seeds[7], 71), 0),
        "log_decay": draw_log_decay(jax.random.fold_in(seeds[7], 71), 0),
        "out_gate": scatter_about(seeds[5], (PROMPT_LENGTH, HV, DV), 1.0, 6.0, ((0, 32),)),
        "norm_gain": jnp.clip(1.0 + 0.18 * jax.random.normal(seeds[6], (DV,), jnp.float32), 0.1, 1.9),
    }


HIGHEST_PREC = lax.Precision.HIGHEST

def unit_rows(matrix):
    return matrix * lax.rsqrt(lax.optimization_barrier(jnp.sum(matrix * matrix, axis=-1, keepdims=True)) + 1e-06)

def block_terms(query_block, key_block, value_block, beta_block, decay_block):
    key_dim = query_block.shape[-1]
    copies = value_block.shape[1] // query_block.shape[1]
    length = query_block.shape[0]
    query_unit = unit_rows(query_block.astype(jnp.float32)) * key_dim ** (-0.5)
    key_unit = unit_rows(key_block.astype(jnp.float32))
    query_heads = jnp.transpose(jnp.repeat(query_unit, copies, axis=1), (1, 0, 2))
    key_heads = jnp.transpose(jnp.repeat(key_unit, copies, axis=1), (1, 0, 2))
    value_heads = jnp.transpose(value_block.astype(jnp.float32), (1, 0, 2))
    beta_rows = jnp.transpose(beta_block)
    cumulative = jnp.cumsum(jnp.transpose(decay_block), axis=1)
    row_ids = lax.broadcasted_iota(jnp.int32, (length, length), 0)
    col_ids = lax.broadcasted_iota(jnp.int32, (length, length), 1)
    inclusive = row_ids >= col_ids
    strict = row_ids > col_ids
    spread = cumulative[:, :, None] - cumulative[:, None, :]
    fading = jnp.where(inclusive, jnp.exp(jnp.where(inclusive, spread, 0.0)), 0.0)
    key_key = jnp.einsum('hid,hjd->hij', key_heads, key_heads, precision=HIGHEST_PREC)
    query_key = jnp.einsum('hid,hjd->hij', query_heads, key_heads, precision=HIGHEST_PREC)
    unit_lower = jnp.where(strict, beta_rows[:, :, None] * fading * key_key, 0.0) + jnp.eye(length, dtype=jnp.float32)
    growth = jnp.exp(cumulative)
    right_cols = jnp.concatenate([(beta_rows * growth)[:, :, None] * key_heads, beta_rows[:, :, None] * value_heads], axis=2)
    solved = lax.linalg.triangular_solve(unit_lower, right_cols, left_side=True, lower=True, unit_diagonal=True)
    weighted_keys = solved[:, :, :key_dim]
    base_values = solved[:, :, key_dim:]
    mixing = fading * query_key
    query_reach = growth[:, :, None] * query_heads - jnp.einsum('hij,hjd->hid', mixing, weighted_keys, precision=HIGHEST_PREC)
    local_rows = jnp.einsum('hij,hjv->hiv', mixing, base_values, precision=HIGHEST_PREC)
    tail_fade = jnp.exp(cumulative[:, -1:] - cumulative)
    tail_keys = tail_fade[:, :, None] * key_heads
    carry_map = growth[:, -1][:, None, None] * jnp.eye(key_dim, dtype=jnp.float32) - jnp.einsum('hcd,hce->hde', weighted_keys, tail_keys, precision=HIGHEST_PREC)
    offset = jnp.einsum('hcv,hcd->hvd', base_values, tail_keys, precision=HIGHEST_PREC)
    return (local_rows, query_reach, carry_map, offset)

def gated_norm(results, out_gate, norm_gain):
    norm_scale = lax.rsqrt(lax.optimization_barrier(jnp.mean(results * results, axis=-1, keepdims=True)) + 1e-06)
    gate_f32 = out_gate.astype(jnp.float32)
    return (results * norm_scale * norm_gain * jax.nn.silu(gate_f32)).astype(jnp.bfloat16)

def reference(queries, keys, values, beta, log_decay, out_gate, norm_gain):
    blocks = queries.shape[0] // BLOCK

    def to_blocks(array):
        return array.reshape((blocks, BLOCK) + array.shape[1:])

    def advance(state_now, pieces):
        local_rows, query_reach, carry_map, offset = block_terms(*pieces)
        results = local_rows + jnp.einsum('hcd,hvd->hcv', query_reach, state_now, precision=HIGHEST_PREC)
        state_next = jnp.einsum('hvd,hde->hve', state_now, carry_map, precision=HIGHEST_PREC) + offset
        return (state_next, jnp.transpose(results, (1, 0, 2)))
    initial = jnp.zeros((HV, DV, DK), jnp.float32)
    pieces = (to_blocks(queries), to_blocks(keys), to_blocks(values), to_blocks(beta), to_blocks(log_decay))
    _, results = lax.scan(advance, initial, pieces)
    results = results.reshape((queries.shape[0], HV, DV))
    return gated_norm(results, out_gate, norm_gain)
```

```python
import functools

import jax
import jax.numpy as jnp
from jax import lax
from jax.experimental import pallas as pl
from jax.experimental.pallas import tpu as pltpu
from jax.sharding import PartitionSpec as P

MESH = pl.DeviceIdType.MESH
F32 = jnp.float32
BF16 = jnp.bfloat16
NN = (((1,), (0,)), ((), ()))
NT = (((1,), (1,)), ((), ()))
TN = (((0,), (0,)), ((), ()))


def dot(a, b, dims=NN):
    return lax.dot_general(a, b, dims, preferred_element_type=F32)


def split(x):
    hi = x.astype(BF16)
    return hi, (x - hi.astype(F32)).astype(BF16)


def cat(parts, axis):
    return jnp.concatenate(parts, axis=axis)


def lhs_pair(x):
    return cat(split(x), 1)


def rhs_square(x):
    both = cat(split(x), 1)
    return cat((both, both), 0)


def mm(lhs, rhs):
    wide = dot(lhs, rhs)
    half = wide.shape[1] // 2
    return wide[:, :half] + wide[:, half:]


def mm_nt(a, b):
    a_hi, a_lo = split(a)
    b_hi, b_lo = split(b)
    return dot(cat((a_hi, a_lo), 1), cat((b_hi, b_hi), 1), NT) + dot(a_hi, b_lo, NT)


def kernel(
    n, steps, heads, bd_hbm, k_hbm, v_hbm, q_hbm, g_hbm, gain_ref, out_ref,
    bd, kb, vb, qb, gb, fade, grow, wu, pairs, prefix, slab, local, reach,
    state_in, state_out, send_sem, recv_sem, chain_send, chain_recv,
):
    me = lax.axis_index("head")
    place = lax.axis_index("seq")
    after = lax.rem(place + 1, steps)
    before = lax.rem(place + steps - 1, steps)
    length, depth = kb.shape[2], kb.shape[3]

    barrier = pltpu.get_barrier_semaphore()
    for d in range(1, n):
        pl.semaphore_signal(
            barrier, inc=1, device_id={"head": lax.rem(me + d, n)}, device_id_type=MESH
        )
    pl.semaphore_signal(barrier, inc=1, device_id={"seq": before}, device_id_type=MESH)
    pl.semaphore_wait(barrier, n)

    sources = (bd_hbm, k_hbm, v_hbm, q_hbm, g_hbm)
    targets = (bd, kb, vb, qb, gb)

    def remote(t, d):
        peer = lax.rem(me + d, n)
        return pltpu.make_async_remote_copy(
            src_ref=sources[t].at[peer],
            dst_ref=targets[t].at[me],
            send_sem=send_sem.at[t, d],
            recv_sem=recv_sem.at[t, n - d],
            device_id={"head": peer},
            device_id_type=MESH,
        )

    def own(t):
        return pltpu.make_async_copy(sources[t].at[me], targets[t].at[me], recv_sem.at[t, 0])

    def arrived(t, d):
        came = lax.rem(me + d, n)
        return pltpu.make_async_remote_copy(
            src_ref=sources[t].at[came],
            dst_ref=targets[t].at[came],
            send_sem=send_sem.at[t, d],
            recv_sem=recv_sem.at[t, d],
            device_id={"head": came},
            device_id_type=MESH,
        )

    for t in range(5):
        own(t).start()
        for d in range(1, n):
            remote(t, d).start()

    def wait_for(t, d):
        @pl.when(d == 0)
        def _():
            own(t).wait()

        @pl.when(d > 0)
        def _():
            arrived(t, d).wait_recv()

    rows = lax.broadcasted_iota(jnp.int32, (length, length), 0)
    cols = lax.broadcasted_iota(jnp.int32, (length, length), 1)
    eye = rows == cols
    inclusive = rows >= cols
    strict = rows > cols
    one = jnp.where(eye, 1.0, 0.0)

    def block_step(d, carry):
        s = lax.rem(me + d, n)
        wait_for(0, d)
        wait_for(1, d)
        keys, lower, scales = [], [], []
        for h in range(heads):
            key = kb[s, h]
            beta_row = bd[s, pl.ds(h, 1), :]
            decay_row = bd[s, pl.ds(heads + h, 1), :]
            cum_col = jnp.sum(jnp.where(inclusive, decay_row, 0.0), axis=1, keepdims=True)
            cum_row = jnp.sum(jnp.where(eye, cum_col, 0.0), axis=0, keepdims=True)
            beta_col = jnp.sum(jnp.where(eye, beta_row, 0.0), axis=1, keepdims=True)
            kk = dot(key, key, NT)
            on_diag = jnp.where(eye, kk, 0.0)
            norm_row = lax.rsqrt(jnp.sum(on_diag, axis=0, keepdims=True) + 1e-06)
            norm_col = lax.rsqrt(jnp.sum(on_diag, axis=1, keepdims=True) + 1e-06)
            fading = jnp.where(
                inclusive, jnp.exp(jnp.where(inclusive, cum_col - cum_row, 0.0)), 0.0
            ) * norm_row
            fade[s, h] = fading
            grow_col = jnp.exp(cum_col)
            grow[s, h] = jnp.broadcast_to(grow_col, (length, depth))
            lower.append(jnp.where(strict, (beta_col * norm_col) * fading * kk, 0.0))
            last = cum_row[:, length - 1 :]
            tail = jnp.exp(last - cum_col) * norm_col
            scales.append((beta_row, beta_row * norm_row * jnp.exp(cum_row), tail, jnp.exp(last)))
            keys.append(key)
        inverse = [one - jnp.where((rows // 2) == (cols // 2), low, 0.0) for low in lower]
        size = 2
        while size < length:
            pick = ((rows // (2 * size)) == (cols // (2 * size))) & (
                (rows // size) != (cols // size)
            )
            crosses = [lhs_pair(jnp.where(pick, low, 0.0)) for low in lower]
            halves = [split(x) for x in inverse]
            lefts = [cat(pair, 1) for pair in halves]
            rights = [cat((left, left), 0) for left in lefts]
            middles = [mm(c, r) for c, r in zip(crosses, rights)]
            products = [mm(l, rhs_square(m)) for l, m in zip(lefts, middles)]
            inverse = [x - p for x, p in zip(inverse, products)]
            size *= 2
        wait_for(2, d)
        for h in range(heads):
            beta_row, key_row, tail, last = scales[h]
            key = keys[h]
            value = vb[s, h]
            w = dot(lhs_pair(inverse[h] * key_row), cat((key, key), 0))
            u = dot(lhs_pair(inverse[h] * beta_row), cat((value, value), 0))
            both = cat((w, u), 1)
            wu[s, h] = both
            hi, lo = split(both * tail)
            moved = dot(cat((hi, lo), 0), cat((key, key), 0), TN)
            pairs[s, h, :depth] = last * one - moved[:depth]
            pairs[s, h, depth:] = moved[depth:]
        return carry

    lax.fori_loop(0, n, block_step, 0)

    for h in range(heads):
        slab[h] = pairs[0, h]

    def compose(s, carry):
        for h in range(heads):
            now = slab[h]
            prefix[s, h] = now
            step = pairs[s, h]
            joined = mm(lhs_pair(now), rhs_square(step[:depth]))
            slab[h, :depth] = joined[:depth]
            slab[h, depth:] = joined[depth:] + step[depth:]
        return carry

    lax.fori_loop(1, n, compose, 0)

    def local_step(d, carry):
        s = lax.rem(me + d, n)
        wait_for(3, d)
        for h in range(heads):
            query = qb[s, h]
            qf = query.astype(F32)
            norm = lax.rsqrt(jnp.sum(qf * qf, axis=1, keepdims=True) + 1e-06) * depth ** (-0.5)
            mixing = dot(query, kb[s, h], NT) * norm * fade[s, h]
            m_hi, m_lo = split(mixing)
            wu_hi, wu_lo = split(wu[s, h])
            mixed = dot(cat((m_hi, m_lo), 1), cat((wu_hi, wu_hi), 0)) + dot(m_hi, wu_lo)
            near = grow[s, h] * (qf * norm) - mixed[:, :depth]
            reach[s, h] = near
            local[s, h] = mixed[:, depth:]

        @pl.when(s > 0)
        def _():
            for h in range(heads):
                joined = mm_nt(reach[s, h], prefix[s, h])
                reach[s, h] = joined[:, :depth]
                local[s, h] += joined[:, depth:]

        return carry

    @pl.when(place >= steps // 2)
    def _():
        lax.fori_loop(0, n, local_step, 0)

    def onward(h):
        return pltpu.make_async_remote_copy(
            src_ref=state_out.at[h],
            dst_ref=state_in.at[h],
            send_sem=chain_send.at[h],
            recv_sem=chain_recv.at[h],
            device_id={"seq": after},
            device_id_type=MESH,
        )

    @pl.when(place == 0)
    def _():
        for h in range(heads):
            state_in[h] = jnp.zeros((depth, depth), F32)
            state_out[h] = slab[h, depth:]
            onward(h).start()

    @pl.when(place > 0)
    def _():
        for h in range(heads):
            right = rhs_square(slab[h, :depth])
            onward(h).wait_recv()
            state_out[h] = mm(lhs_pair(state_in[h]), right) + slab[h, depth:]

            @pl.when(place < steps - 1)
            def _():
                onward(h).start()

    @pl.when(place < steps // 2)
    def _():
        lax.fori_loop(0, n, local_step, 0)

    gain = gain_ref[...]

    def finish(d, carry):
        s = lax.rem(me + d, n)
        wait_for(4, d)
        for h in range(heads):
            result = local[s, h] + mm_nt(reach[s, h], state_in[h])
            scale = lax.rsqrt(jnp.mean(result * result, axis=1, keepdims=True) + 1e-06)
            gate = gb[s, h].astype(F32)
            gated = result * scale * gain * (gate / (1.0 + jnp.exp(-gate)))
            out_ref[h, pl.ds(pl.multiple_of(s * length, length), length), :] = gated.astype(BF16)
        return carry

    lax.fori_loop(0, n, finish, 0)

    for t in range(5):
        for d in range(1, n):
            remote(t, d).wait_send()

    @pl.when(place < steps - 1)
    def _():
        for h in range(heads):
            onward(h).wait_send()


def body(n, steps, queries, keys, values, beta, log_decay, out_gate, norm_gain):
    length, all_heads, depth = keys.shape
    heads = all_heads // n

    def regroup(x):
        return jnp.transpose(x.reshape(length, n, heads, depth), (1, 2, 0, 3))

    def rows_of(x):
        return jnp.transpose(x).reshape(n, heads, length)

    padded = -(-2 * heads // 8) * 8
    bd = jnp.concatenate(
        [rows_of(beta), rows_of(log_decay), jnp.zeros((n, padded - 2 * heads, length), F32)], axis=1
    )
    big = (n, heads, length, depth)
    any_spec = pl.BlockSpec(memory_space=pl.ANY)
    vmem = pl.BlockSpec(memory_space=pltpu.VMEM)
    out = pl.pallas_call(
        functools.partial(kernel, n, steps, heads),
        out_shape=jax.ShapeDtypeStruct((heads, n * length, depth), BF16),
        in_specs=[any_spec] * 5 + [vmem],
        out_specs=vmem,
        scratch_shapes=[
            pltpu.VMEM((n, padded, length), F32),
            pltpu.VMEM(big, BF16),
            pltpu.VMEM(big, BF16),
            pltpu.VMEM(big, BF16),
            pltpu.VMEM(big, BF16),
            pltpu.VMEM((n, heads, length, length), F32),
            pltpu.VMEM(big, F32),
            pltpu.VMEM((n, heads, length, 2 * depth), F32),
            pltpu.VMEM((n, heads, 2 * depth, depth), F32),
            pltpu.VMEM((n, heads, 2 * depth, depth), F32),
            pltpu.VMEM((heads, 2 * depth, depth), F32),
            pltpu.VMEM(big, F32),
            pltpu.VMEM(big, F32),
            pltpu.VMEM((heads, depth, depth), F32),
            pltpu.VMEM((heads, depth, depth), F32),
            pltpu.SemaphoreType.DMA((5, n)),
            pltpu.SemaphoreType.DMA((5, n)),
            pltpu.SemaphoreType.DMA((heads,)),
            pltpu.SemaphoreType.DMA((heads,)),
        ],
        compiler_params=pltpu.CompilerParams(
            collective_id=0, has_side_effects=True, vmem_limit_bytes=48 * 1024 * 1024
        ),
    )(bd, regroup(keys), regroup(values), regroup(queries), regroup(out_gate), norm_gain[None, :])
    return jnp.transpose(out, (1, 0, 2))


def solution(mesh):
    return jax.shard_map(
        functools.partial(body, mesh.shape["head"], mesh.shape["seq"]),
        mesh=mesh,
        in_specs=(
            P(("seq", "head"), None, None),
            P(("seq", "head"), None, None),
            P(("seq", "head"), None, None),
            P(("seq", "head"), None),
            P(("seq", "head"), None),
            P(("seq", "head"), None, None),
            P(),
        ),
        out_specs=P("seq", "head", None),
        check_vma=False,
    )
```

```python
import functools

import jax
import jax.numpy as jnp
from jax import lax
from jax.experimental import pallas as pl
from jax.experimental.pallas import tpu as pltpu
from jax.sharding import PartitionSpec as P

MESH = pl.DeviceIdType.MESH
F32 = jnp.float32
BF16 = jnp.bfloat16
NN = (((1,), (0,)), ((), ()))
NT = (((1,), (1,)), ((), ()))
TN = (((0,), (0,)), ((), ()))


def dot(a, b, dims=NN):
    return lax.dot_general(a, b, dims, preferred_element_type=F32)


def split(x):
    hi = x.astype(BF16)
    return hi, (x - hi.astype(F32)).astype(BF16)


def cat(parts, axis):
    return jnp.concatenate(parts, axis=axis)


def lhs_pair(x):
    return cat(split(x), 1)


def rhs_square(x):
    both = cat(split(x), 1)
    return cat((both, both), 0)


def mm(lhs, rhs):
    wide = dot(lhs, rhs)
    half = wide.shape[1] // 2
    return wide[:, :half] + wide[:, half:]


def mm_nt(a, b):
    a_hi, a_lo = split(a)
    b_hi, b_lo = split(b)
    return dot(cat((a_hi, a_lo), 1), cat((b_hi, b_hi), 1), NT) + dot(a_hi, b_lo, NT)


def partner(me, d, n):
    if n & (n - 1):
        return lax.rem(2 * n + d - me, n)
    found, bit = 0, 1
    while bit < n:
        found += lax.rem(me // bit + d // bit, 2) * bit
        bit *= 2
    return found


def kernel(
    n, steps, heads, beta_hbm, decay_hbm, k_hbm, v_hbm, q_hbm, g_hbm, gain_hbm, out_ref,
    betas, decays, kb, vb, qb, gb, gain_ref, fade, grow, tails, solved, wu, pairs, prefix, slab,
    local, reach, state_in, state_out, send_sem, recv_sem, chain_send, chain_recv, gain_sem,
):
    me = lax.axis_index("head")
    place = lax.axis_index("seq")
    after = lax.rem(place + 1, steps)
    before = lax.rem(place + steps - 1, steps)
    length, depth = kb.shape[1], kb.shape[3]

    barrier = pltpu.get_barrier_semaphore()
    for d in range(1, n):
        pl.semaphore_signal(
            barrier, inc=1, device_id={"head": partner(me, d, n)}, device_id_type=MESH
        )
    pl.semaphore_signal(barrier, inc=1, device_id={"seq": before}, device_id_type=MESH)
    pl.semaphore_wait(barrier, n)

    sources = (beta_hbm, decay_hbm, k_hbm, v_hbm, q_hbm, g_hbm)
    targets = (betas, decays, kb, vb, qb, gb)
    kinds = len(sources)

    def part(t, peer):
        return sources[t].at[peer] if t < 2 else sources[t].at[:, peer]

    def remote(t, d):
        peer = partner(me, d, n)
        return pltpu.make_async_remote_copy(
            src_ref=part(t, peer),
            dst_ref=targets[t].at[me],
            send_sem=send_sem.at[t, d],
            recv_sem=recv_sem.at[t, d],
            device_id={"head": peer},
            device_id_type=MESH,
        )

    def own(t):
        return pltpu.make_async_copy(part(t, me), targets[t].at[me], recv_sem.at[t, 0])

    for t in range(kinds):
        own(t).start()
        for d in range(1, n):
            remote(t, d).start()
    pltpu.make_async_copy(gain_hbm, gain_ref, gain_sem).start()

    def wait_for(t, d):
        @pl.when(d == 0)
        def _():
            own(t).wait()

        @pl.when(d > 0)
        def _():
            remote(t, d).wait_recv()

    rows = lax.broadcasted_iota(jnp.int32, (length, length), 0)
    cols = lax.broadcasted_iota(jnp.int32, (length, length), 1)
    eye = rows == cols
    inclusive = rows >= cols
    strict = rows > cols
    one = jnp.where(eye, 1.0, 0.0)

    def heads_of(ref, s):
        return jnp.swapaxes(ref[s], 0, 1)

    group = 2 if n % 2 == 0 else 1

    def key_step(step, carry):
        lower, marks = [], []
        for j in range(group):
            d = step * group + j
            s = partner(me, d, n)
            for t in range(3):
                wait_for(t, d)
            keys = heads_of(kb, s)
            for h in range(heads):
                key = keys[h]
                beta_row = betas[s, pl.ds(h, 1), :]
                decay_row = decays[s, pl.ds(h, 1), :]
                cum_col = jnp.sum(jnp.where(inclusive, decay_row, 0.0), axis=1, keepdims=True)
                cum_row = jnp.sum(jnp.where(eye, cum_col, 0.0), axis=0, keepdims=True)
                beta_col = jnp.sum(jnp.where(eye, beta_row, 0.0), axis=1, keepdims=True)
                kk = dot(key, key, NT)
                on_diag = jnp.where(eye, kk, 0.0)
                norm_row = lax.rsqrt(jnp.sum(on_diag, axis=0, keepdims=True) + 1e-06)
                norm_col = lax.rsqrt(jnp.sum(on_diag, axis=1, keepdims=True) + 1e-06)
                fading = jnp.where(
                    inclusive, jnp.exp(jnp.where(inclusive, cum_col - cum_row, 0.0)), 0.0
                ) * norm_row
                fade[s, h] = fading
                grow[s, h] = jnp.broadcast_to(jnp.exp(cum_col), (length, depth))
                tail = jnp.exp(cum_row[:, length - 1 :] - cum_col) * norm_col
                tails[s, h] = jnp.broadcast_to(tail, (length, depth))
                lower.append(jnp.where(strict, (beta_col * norm_col) * fading * kk, 0.0))
                marks.append((s, h, key, beta_row, beta_row * norm_row * jnp.exp(cum_row)))
        inverse = [one - jnp.where((rows // 2) == (cols // 2), low, 0.0) for low in lower]
        size = 2
        while size < length:
            pick = ((rows // (2 * size)) == (cols // (2 * size))) & (
                (rows // size) != (cols // size)
            )
            crosses = [lhs_pair(jnp.where(pick, low, 0.0)) for low in lower]
            lefts = [lhs_pair(x) for x in inverse]
            middles = [mm(c, cat((left, left), 0)) for c, left in zip(crosses, lefts)]
            products = [mm(left, rhs_square(m)) for left, m in zip(lefts, middles)]
            inverse = [x - p for x, p in zip(inverse, products)]
            size *= 2
        for x, (s, h, key, beta_row, key_row) in zip(inverse, marks):
            wu[s, h, :, :depth] = dot(lhs_pair(x * key_row), cat((key, key), 0))
            solved[s, h] = lhs_pair(x * beta_row)
        return carry

    lax.fori_loop(0, n // group, key_step, 0)

    def value_step(d, carry):
        s = partner(me, d, n)
        wait_for(3, d)
        keys = heads_of(kb, s)
        values = heads_of(vb, s)
        for h in range(heads):
            key, value = keys[h], values[h]
            u = dot(solved[s, h], cat((value, value), 0))
            wu[s, h, :, depth:] = u
            tail = tails[s, h]
            hi, lo = split(cat((wu[s, h, :, :depth] * tail, u * tail), 1))
            moved = dot(cat((hi, lo), 0), cat((key, key), 0), TN)
            pairs[s, h, :depth] = grow[s, h, length - 1 :, :] * one - moved[:depth]
            pairs[s, h, depth:] = moved[depth:]
        return carry

    lax.fori_loop(0, n, value_step, 0)

    for h in range(heads):
        slab[h] = pairs[0, h]

    def compose(s, carry):
        for h in range(heads):
            now = slab[h]
            prefix[s, h] = now
            step = pairs[s, h]
            joined = mm(lhs_pair(now), rhs_square(step[:depth]))
            slab[h, :depth] = joined[:depth]
            slab[h, depth:] = joined[depth:] + step[depth:]
        return carry

    lax.fori_loop(1, n, compose, 0)

    def local_step(d, carry):
        s = partner(me, d, n)
        wait_for(4, d)
        keys = heads_of(kb, s)
        queries = heads_of(qb, s)
        for h in range(heads):
            query = queries[h]
            qf = query.astype(F32)
            norm = lax.rsqrt(jnp.sum(qf * qf, axis=1, keepdims=True) + 1e-06) * depth ** (-0.5)
            mixing = dot(query, keys[h], NT) * norm * fade[s, h]
            m_hi, m_lo = split(mixing)
            wu_hi, wu_lo = split(wu[s, h])
            mixed = dot(cat((m_hi, m_lo), 1), cat((wu_hi, wu_hi), 0)) + dot(m_hi, wu_lo)
            near = grow[s, h] * (qf * norm) - mixed[:, :depth]
            reach[s, h] = near
            local[s, h] = mixed[:, depth:]

        @pl.when(s > 0)
        def _():
            for h in range(heads):
                joined = mm_nt(reach[s, h], prefix[s, h])
                reach[s, h] = joined[:, :depth]
                local[s, h] += joined[:, depth:]

        return carry

    @pl.when(place > steps // 2)
    def _():
        lax.fori_loop(0, n, local_step, 0)

    cuts = chain_send.shape[1]
    rows_cut = depth // cuts

    def onward(h, c):
        return pltpu.make_async_remote_copy(
            src_ref=state_out.at[h, pl.ds(c * rows_cut, rows_cut)],
            dst_ref=state_in.at[h, pl.ds(c * rows_cut, rows_cut)],
            send_sem=chain_send.at[h, c],
            recv_sem=chain_recv.at[h, c],
            device_id={"seq": after},
            device_id_type=MESH,
        )

    @pl.when(place == 0)
    def _():
        for h in range(heads):
            state_in[h] = jnp.zeros((depth, depth), F32)
            state_out[h] = slab[h, depth:]
            for c in range(cuts):
                onward(h, c).start()

    @pl.when(place > 0)
    def _():
        for h in range(heads):
            right = rhs_square(slab[h, :depth])
            for c in range(cuts):
                piece = pl.ds(c * rows_cut, rows_cut)
                onward(h, c).wait_recv()
                state_out[h, piece] = (
                    mm(lhs_pair(state_in[h, piece]), right)
                    + slab[h, pl.ds(depth + c * rows_cut, rows_cut)]
                )

                @pl.when(place < steps - 1)
                def _():
                    onward(h, c).start()

    @pl.when(place <= steps // 2)
    def _():
        lax.fori_loop(0, n, local_step, 0)

    pltpu.make_async_copy(gain_hbm, gain_ref, gain_sem).wait()
    gain = gain_ref[...]

    def finish(d, carry):
        s = partner(me, d, n)
        wait_for(5, d)
        gates = heads_of(gb, s)
        for h in range(heads):
            result = local[s, h] + mm_nt(reach[s, h], state_in[h])
            scale = lax.rsqrt(jnp.mean(result * result, axis=1, keepdims=True) + 1e-06)
            gate = gates[h].astype(F32)
            gated = result * scale * gain * (gate / (1.0 + jnp.exp(-gate)))
            out_ref[h, pl.ds(pl.multiple_of(s * length, length), length), :] = gated.astype(BF16)
        return carry

    lax.fori_loop(0, n, finish, 0)

    for t in range(kinds):
        for d in range(1, n):
            remote(t, d).wait_send()

    @pl.when(place < steps - 1)
    def _():
        for h in range(heads):
            for c in range(cuts):
                onward(h, c).wait_send()


def body(n, steps, queries, keys, values, beta, log_decay, out_gate, norm_gain):
    length, all_heads, depth = keys.shape
    heads = all_heads // n

    cuts = 2 if depth % 16 == 0 else 1

    def grouped(x):
        return x.reshape(length, n, heads, depth)

    def rows_of(x):
        return jnp.transpose(x).reshape(n, heads, length)

    raw = (n, length, heads, depth)
    big = (n, heads, length, depth)
    tall = (n, heads, 2 * depth, depth)
    out = pl.pallas_call(
        functools.partial(kernel, n, steps, heads),
        out_shape=jax.ShapeDtypeStruct((heads, n * length, depth), BF16),
        in_specs=[pl.BlockSpec(memory_space=pl.ANY)] * 7,
        out_specs=pl.BlockSpec(memory_space=pltpu.VMEM),
        scratch_shapes=[
            pltpu.VMEM((n, heads, length), F32),
            pltpu.VMEM((n, heads, length), F32),
            pltpu.VMEM(raw, BF16),
            pltpu.VMEM(raw, BF16),
            pltpu.VMEM(raw, BF16),
            pltpu.VMEM(raw, BF16),
            pltpu.VMEM((1, depth), F32),
            pltpu.VMEM((n, heads, length, length), F32),
            pltpu.VMEM(big, F32),
            pltpu.VMEM(big, F32),
            pltpu.VMEM((n, heads, length, 2 * length), BF16),
            pltpu.VMEM((n, heads, length, 2 * depth), F32),
            pltpu.VMEM(tall, F32),
            pltpu.VMEM(tall, F32),
            pltpu.VMEM((heads, 2 * depth, depth), F32),
            pltpu.VMEM(big, F32),
            pltpu.VMEM(big, F32),
            pltpu.VMEM((heads, depth, depth), F32),
            pltpu.VMEM((heads, depth, depth), F32),
            pltpu.SemaphoreType.DMA((6, n)),
            pltpu.SemaphoreType.DMA((6, n)),
            pltpu.SemaphoreType.DMA((heads, cuts)),
            pltpu.SemaphoreType.DMA((heads, cuts)),
            pltpu.SemaphoreType.DMA,
        ],
        compiler_params=pltpu.CompilerParams(
            collective_id=0, has_side_effects=True, vmem_limit_bytes=67043328
        ),
    )(
        rows_of(beta),
        rows_of(log_decay),
        grouped(keys),
        grouped(values),
        grouped(queries),
        grouped(out_gate),
        norm_gain[None, :],
    )
    return jnp.transpose(out, (1, 0, 2))


def solution(mesh):
    return jax.shard_map(
        functools.partial(body, mesh.shape["head"], mesh.shape["seq"]),
        mesh=mesh,
        in_specs=(
            P(("seq", "head"), None, None),
            P(("seq", "head"), None, None),
            P(("seq", "head"), None, None),
            P(("seq", "head"), None),
            P(("seq", "head"), None),
            P(("seq", "head"), None, None),
            P(),
        ),
        out_specs=P("seq", "head", None),
        check_vma=False,
    )
```

```python
import functools

import jax
import jax.numpy as jnp
from jax import lax
from jax.experimental import pallas as pl
from jax.experimental.pallas import tpu as pltpu
from jax.sharding import PartitionSpec as P

MESH = pl.DeviceIdType.MESH
F32 = jnp.float32
BF16 = jnp.bfloat16
NN = (((1,), (0,)), ((), ()))
NT = (((1,), (1,)), ((), ()))
TN = (((0,), (0,)), ((), ()))


def dot(a, b, dims=NN):
    return lax.dot_general(a, b, dims, preferred_element_type=F32)


def split(x):
    hi = x.astype(BF16)
    return hi, (x - hi.astype(F32)).astype(BF16)


def cat(parts, axis):
    return jnp.concatenate(parts, axis=axis)


def lhs_pair(x):
    return cat(split(x), 1)


def rhs_square(x):
    both = cat(split(x), 1)
    return cat((both, both), 0)


def mm(lhs, rhs):
    wide = dot(lhs, rhs)
    half = wide.shape[1] // 2
    return wide[:, :half] + wide[:, half:]


def mm_nt(a, b):
    a_hi, a_lo = split(a)
    b_hi, b_lo = split(b)
    return dot(cat((a_hi, a_lo), 1), cat((b_hi, b_hi), 1), NT) + dot(a_hi, b_lo, NT)


def partner(me, d, n):
    if n & (n - 1):
        return lax.rem(2 * n + d - me, n)
    found, bit = 0, 1
    while bit < n:
        found += lax.rem(me // bit + d // bit, 2) * bit
        bit *= 2
    return found


def kernel(
    n, steps, heads, beta_hbm, decay_hbm, k_hbm, v_hbm, q_hbm, g_hbm, gain_hbm, out_ref,
    betas, decays, kb, vb, qb, gb, gain_ref, factors, fade, grow, tails, solved, wu, pairs, prefix, slab,
    local, reach, state_in, state_out, send_sem, recv_sem, chain_send, chain_recv, gain_sem,
):
    me = lax.axis_index("head")
    place = lax.axis_index("seq")
    after = lax.rem(place + 1, steps)
    before = lax.rem(place + steps - 1, steps)
    length, depth = kb.shape[1], kb.shape[3]

    barrier = pltpu.get_barrier_semaphore()
    for d in range(1, n):
        pl.semaphore_signal(
            barrier, inc=1, device_id={"head": partner(me, d, n)}, device_id_type=MESH
        )
    pl.semaphore_signal(barrier, inc=1, device_id={"seq": before}, device_id_type=MESH)
    pl.semaphore_wait(barrier, n)

    sources = (beta_hbm, decay_hbm, k_hbm, v_hbm, q_hbm, g_hbm)
    targets = (betas, decays, kb, vb, qb, gb)
    kinds = len(sources)

    def part(t, peer):
        return sources[t].at[peer] if t < 2 else sources[t].at[:, peer]

    def remote(t, d):
        peer = partner(me, d, n)
        return pltpu.make_async_remote_copy(
            src_ref=part(t, peer),
            dst_ref=targets[t].at[me],
            send_sem=send_sem.at[t, d],
            recv_sem=recv_sem.at[t, d],
            device_id={"head": peer},
            device_id_type=MESH,
        )

    def own(t):
        return pltpu.make_async_copy(part(t, me), targets[t].at[me], recv_sem.at[t, 0])

    for t in range(kinds):
        own(t).start()
        for d in range(1, n):
            remote(t, d).start()
    pltpu.make_async_copy(gain_hbm, gain_ref, gain_sem).start()

    def wait_for(t, d):
        @pl.when(d == 0)
        def _():
            own(t).wait()

        @pl.when(d > 0)
        def _():
            remote(t, d).wait_recv()

    rows = lax.broadcasted_iota(jnp.int32, (length, length), 0)
    cols = lax.broadcasted_iota(jnp.int32, (length, length), 1)
    eye = rows == cols
    inclusive = rows >= cols
    strict = rows > cols
    one = jnp.where(eye, 1.0, 0.0)

    def heads_of(ref, s):
        return jnp.swapaxes(ref[s], 0, 1)

    group = 2 if n % 2 == 0 else 1

    def key_step(step, carry):
        lower, marks = [], []
        for j in range(group):
            d = step * group + j
            s = partner(me, d, n)
            for t in range(3):
                wait_for(t, d)
            keys = heads_of(kb, s)
            for h in range(heads):
                key = keys[h]
                beta_row = betas[s, pl.ds(h, 1), :]
                decay_row = decays[s, pl.ds(h, 1), :]
                cum_col = jnp.sum(jnp.where(inclusive, decay_row, 0.0), axis=1, keepdims=True)
                cum_row = jnp.sum(jnp.where(eye, cum_col, 0.0), axis=0, keepdims=True)
                beta_col = jnp.sum(jnp.where(eye, beta_row, 0.0), axis=1, keepdims=True)
                kk = dot(key, key, NT)
                on_diag = jnp.where(eye, kk, 0.0)
                norm_row = lax.rsqrt(jnp.sum(on_diag, axis=0, keepdims=True) + 1e-06)
                norm_col = lax.rsqrt(jnp.sum(on_diag, axis=1, keepdims=True) + 1e-06)
                fading = jnp.where(
                    inclusive, jnp.exp(jnp.where(inclusive, cum_col - cum_row, 0.0)), 0.0
                ) * norm_row
                fade[s, h] = fading
                grow[s, h] = jnp.broadcast_to(jnp.exp(cum_col), (length, depth))
                tail = jnp.exp(cum_row[:, length - 1 :] - cum_col) * norm_col
                tails[s, h] = jnp.broadcast_to(tail, (length, depth))
                lower.append(jnp.where(strict, (beta_col * norm_col) * fading * kk, 0.0))
                marks.append((s, h, key, beta_row, beta_row * norm_row * jnp.exp(cum_row)))
        inverse = [one - jnp.where((rows // 2) == (cols // 2), low, 0.0) for low in lower]
        size = 2
        while size < length:
            pick = ((rows // (2 * size)) == (cols // (2 * size))) & (
                (rows // size) != (cols // size)
            )
            crosses = [lhs_pair(jnp.where(pick, low, 0.0)) for low in lower]
            lefts = [lhs_pair(x) for x in inverse]
            middles = [mm(c, cat((left, left), 0)) for c, left in zip(crosses, lefts)]
            products = [mm(left, rhs_square(m)) for left, m in zip(lefts, middles)]
            inverse = [x - p for x, p in zip(inverse, products)]
            size *= 2
        for x, (s, h, key, beta_row, key_row) in zip(inverse, marks):
            wu[s, h, :, :depth] = dot(lhs_pair(x * key_row), cat((key, key), 0))
            solved[s, h] = lhs_pair(x * beta_row)
        return carry

    lax.fori_loop(0, n // group, key_step, 0)

    def value_step(step, carry):
        found = []
        for j in range(group):
            s = partner(me, step * group + j, n)
            wait_for(3, step * group + j)
            keys = heads_of(kb, s)
            values = heads_of(vb, s)
            found += [(s, h, keys[h], values[h]) for h in range(heads)]
        us = [dot(solved[s, h], cat((value, value), 0)) for s, h, _, value in found]
        both = [
            cat((wu[s, h, :, :depth] * tails[s, h], u * tails[s, h]), 1)
            for u, (s, h, _, _) in zip(us, found)
        ]
        moves = [
            dot(cat(split(b), 0), cat((key, key), 0), TN)
            for b, (_, _, key, _) in zip(both, found)
        ]
        for u, moved, (s, h, _, _) in zip(us, moves, found):
            wu[s, h, :, depth:] = u
            pairs[s, h, :depth] = grow[s, h, length - 1 :, :] * one - moved[:depth]
            pairs[s, h, depth:] = moved[depth:]
        return carry

    lax.fori_loop(0, n // group, value_step, 0)

    for h in range(heads):
        slab[h] = pairs[0, h]

    def compose(s, carry):
        for h in range(heads):
            now = slab[h]
            prefix[s, h] = now
            step = pairs[s, h]
            joined = mm(lhs_pair(now), rhs_square(step[:depth]))
            slab[h, :depth] = joined[:depth]
            slab[h, depth:] = joined[depth:] + step[depth:]
        return carry

    lax.fori_loop(1, n, compose, 0)

    def local_step(d, carry):
        s = partner(me, d, n)
        wait_for(4, d)
        keys = heads_of(kb, s)
        queries = heads_of(qb, s)
        for h in range(heads):
            query = queries[h]
            qf = query.astype(F32)
            norm = lax.rsqrt(jnp.sum(qf * qf, axis=1, keepdims=True) + 1e-06) * depth ** (-0.5)
            mixing = dot(query, keys[h], NT) * norm * fade[s, h]
            m_hi, m_lo = split(mixing)
            wu_hi, wu_lo = split(wu[s, h])
            mixed = dot(cat((m_hi, m_lo), 1), cat((wu_hi, wu_hi), 0)) + dot(m_hi, wu_lo)
            near = grow[s, h] * (qf * norm) - mixed[:, :depth]
            reach[s, h] = near
            local[s, h] = mixed[:, depth:]

        @pl.when(s > 0)
        def _():
            for h in range(heads):
                joined = mm_nt(reach[s, h], prefix[s, h])
                reach[s, h] = joined[:, :depth]
                local[s, h] += joined[:, depth:]

        return carry

    @pl.when(place >= steps // 2)
    def _():
        lax.fori_loop(0, n, local_step, 0)

    pltpu.make_async_copy(gain_hbm, gain_ref, gain_sem).wait()
    gain = gain_ref[...]

    def gate_step(d, carry):
        s = partner(me, d, n)
        wait_for(5, d)
        gates = heads_of(gb, s)
        for h in range(heads):
            gate = gates[h].astype(F32)
            factors[s, h] = gain * (gate / (1.0 + jnp.exp(-gate)))
        return carry

    @pl.when(place >= steps - 2)
    def _():
        lax.fori_loop(0, n, gate_step, 0)

    cuts = chain_send.shape[1]
    rows_cut = depth // cuts

    def onward(h, c):
        return pltpu.make_async_remote_copy(
            src_ref=state_out.at[h, pl.ds(c * rows_cut, rows_cut)],
            dst_ref=state_in.at[h, pl.ds(c * rows_cut, rows_cut)],
            send_sem=chain_send.at[h, c],
            recv_sem=chain_recv.at[h, c],
            device_id={"seq": after},
            device_id_type=MESH,
        )

    @pl.when(place == 0)
    def _():
        for h in range(heads):
            state_in[h] = jnp.zeros((depth, depth), F32)
            state_out[h] = slab[h, depth:]
            for c in range(cuts):
                onward(h, c).start()

    @pl.when(place > 0)
    def _():
        for h in range(heads):
            right = rhs_square(slab[h, :depth])
            for c in range(cuts):
                piece = pl.ds(c * rows_cut, rows_cut)
                onward(h, c).wait_recv()
                state_out[h, piece] = (
                    mm(lhs_pair(state_in[h, piece]), right)
                    + slab[h, pl.ds(depth + c * rows_cut, rows_cut)]
                )

                @pl.when(place < steps - 1)
                def _():
                    onward(h, c).start()

    @pl.when(place < steps // 2)
    def _():
        lax.fori_loop(0, n, local_step, 0)

    @pl.when(place < steps - 2)
    def _():
        lax.fori_loop(0, n, gate_step, 0)

    def finish(d, carry):
        s = partner(me, d, n)
        for h in range(heads):
            result = local[s, h] + mm_nt(reach[s, h], state_in[h])
            scale = lax.rsqrt(jnp.mean(result * result, axis=1, keepdims=True) + 1e-06)
            gated = result * scale * factors[s, h]
            out_ref[h, pl.ds(pl.multiple_of(s * length, length), length), :] = gated.astype(BF16)
        return carry

    lax.fori_loop(0, n, finish, 0)

    for t in range(kinds):
        for d in range(1, n):
            remote(t, d).wait_send()

    @pl.when(place < steps - 1)
    def _():
        for h in range(heads):
            for c in range(cuts):
                onward(h, c).wait_send()


def body(n, steps, queries, keys, values, beta, log_decay, out_gate, norm_gain):
    length, all_heads, depth = keys.shape
    heads = all_heads // n

    cuts = 4 if depth % 32 == 0 else 1

    def grouped(x):
        return x.reshape(length, n, heads, depth)

    def rows_of(x):
        return jnp.transpose(x).reshape(n, heads, length)

    raw = (n, length, heads, depth)
    big = (n, heads, length, depth)
    tall = (n, heads, 2 * depth, depth)
    out = pl.pallas_call(
        functools.partial(kernel, n, steps, heads),
        out_shape=jax.ShapeDtypeStruct((heads, n * length, depth), BF16),
        in_specs=[pl.BlockSpec(memory_space=pl.ANY)] * 7,
        out_specs=pl.BlockSpec(memory_space=pltpu.VMEM),
        scratch_shapes=[
            pltpu.VMEM((n, heads, length), F32),
            pltpu.VMEM((n, heads, length), F32),
            pltpu.VMEM(raw, BF16),
            pltpu.VMEM(raw, BF16),
            pltpu.VMEM(raw, BF16),
            pltpu.VMEM(raw, BF16),
            pltpu.VMEM((1, depth), F32),
            pltpu.VMEM(big, F32),
            pltpu.VMEM((n, heads, length, length), F32),
            pltpu.VMEM(big, F32),
            pltpu.VMEM(big, F32),
            pltpu.VMEM((n, heads, length, 2 * length), BF16),
            pltpu.VMEM((n, heads, length, 2 * depth), F32),
            pltpu.VMEM(tall, F32),
            pltpu.VMEM(tall, F32),
            pltpu.VMEM((heads, 2 * depth, depth), F32),
            pltpu.VMEM(big, F32),
            pltpu.VMEM(big, F32),
            pltpu.VMEM((heads, depth, depth), F32),
            pltpu.VMEM((heads, depth, depth), F32),
            pltpu.SemaphoreType.DMA((6, n)),
            pltpu.SemaphoreType.DMA((6, n)),
            pltpu.SemaphoreType.DMA((heads, cuts)),
            pltpu.SemaphoreType.DMA((heads, cuts)),
            pltpu.SemaphoreType.DMA,
        ],
        compiler_params=pltpu.CompilerParams(
            collective_id=0, has_side_effects=True, vmem_limit_bytes=67043328
        ),
    )(
        rows_of(beta),
        rows_of(log_decay),
        grouped(keys),
        grouped(values),
        grouped(queries),
        grouped(out_gate),
        norm_gain[None, :],
    )
    return jnp.transpose(out, (1, 0, 2))


def solution(mesh):
    return jax.shard_map(
        functools.partial(body, mesh.shape["head"], mesh.shape["seq"]),
        mesh=mesh,
        in_specs=(
            P(("seq", "head"), None, None),
            P(("seq", "head"), None, None),
            P(("seq", "head"), None, None),
            P(("seq", "head"), None),
            P(("seq", "head"), None),
            P(("seq", "head"), None, None),
            P(),
        ),
        out_specs=P("seq", "head", None),
        check_vma=False,
    )
```
